256 devices in a mesh: zero: 32 (over z, y), tp: 8 (over x, core).
Axes of the slice: x: 4, y: 4, z: 8, core: 2. Of those that a mesh axis runs over, the one named last changes fastest.
Arguments:
- train_gate: bfloat16 [3072, 8192], P('zero', 'tp'), may hold values from -0.109375 to 0.109375
- low_gate: bfloat16 [3072, 16], P('zero'), may hold values from -0.109375 to 0.109375
- high_gate: bfloat16 [16, 8192], P(None, 'tp'), may hold values from -1.5 to 1.5
- train_up: bfloat16 [3072, 8192], P('zero', 'tp'), may hold values from -0.109375 to 0.109375
- low_up: bfloat16 [3072, 16], P('zero'), may hold values from -0.109375 to 0.109375
- high_up: bfloat16 [16, 8192], P(None, 'tp'), may hold values from -1.5 to 1.5
- train_down: bfloat16 [8192, 3072], P('tp', 'zero'), may hold values from -0.0625 to 0.0625
- low_down: bfloat16 [8192, 16], P('tp'), may hold values from -0.0625 to 0.0625
- high_down: bfloat16 [16, 3072], P(None, 'zero'), may hold values from -1.5 to 1.5
- norm_train: float32 [3072], P(('zero', 'tp')), may hold values from 0.25 to 1.75
- norm_step: float32 [3072], P(('zero', 'tp')), may hold values from -0.3 to 0.3
Outputs:
- serve_gate: bfloat16 [8192, 3072], P('tp')
- serve_up: bfloat16 [8192, 3072], P('tp')
- serve_down: bfloat16 [3072, 8192], P(None, 'tp')
- serve_norm: bfloat16 [3072], replicated
The draws below stay inside these ranges and needn't reach their ends.
All inputs are finite; a program needn't handle non-finite values.
Results may differ from the reference program's by a relative error of at most 0.001.
Values may be sent and summed in bfloat16 or wider, within the bound.
No kernel may reach another device: no remote copies, remote signals or barrier semaphores. Data moves between devices by JAX's collectives and lax.ppermute only.
A program may use at most 128 MiB of HBM per device.

```python
import jax
import jax.numpy as jnp

D_MODEL = 3072
D_INNER = 8192
RANK = 16


def block_levels(stream_key, dims, cuts, low, top_value):
    level, own = 1.0, jax.random.fold_in(stream_key, 6)
    for position, parts in cuts:
        draws = jnp.exp(jax.random.uniform(jax.random.fold_in(own, position), (parts,), jnp.float32, low / len(cuts), top_value / len(cuts)))
        level = level * jnp.repeat(draws, dims[position] // parts).reshape([-1 if axis == position else 1 for axis in range(len(dims))])
    return level


def normal_values(own_key, extent, deviation, most, shards=(), dtype=jnp.bfloat16):
    loudness = block_levels(own_key, extent, shards, -0.22, 0.18) if shards else 1.0
    values = jax.random.normal(own_key, extent, jnp.float32) * deviation * loudness
    return jnp.minimum(jnp.maximum(values, -most), most).astype(dtype)


def setup_inputs(seed: int = 0) -> dict:
    splits = jax.random.split(jax.random.key(seed), 12)
    return {
        "train_gate": normal_values(splits[0], (D_MODEL, D_INNER), D_MODEL ** -0.5, 0.109375, ((0, 32), (1, 8))),
        "low_gate": normal_values(splits[1], (D_MODEL, RANK), D_MODEL ** -0.5, 0.109375, ((0, 32),)),
        "high_gate": normal_values(splits[2], (RANK, D_INNER), RANK ** -0.5, 1.5, ((1, 8),)),
        "train_up": normal_values(splits[3], (D_MODEL, D_INNER), D_MODEL ** -0.5, 0.109375, ((0, 32), (1, 8))),
        "low_up": normal_values(splits[4], (D_MODEL, RANK), D_MODEL ** -0.5, 0.109375, ((0, 32),)),
        "high_up": normal_values(splits[5], (RANK, D_INNER), RANK ** -0.5, 1.5, ((1, 8),)),
        "train_down": normal_values(splits[6], (D_INNER, D_MODEL), D_INNER ** -0.5, 0.0625, ((0, 8), (1, 32))),
        "low_down": normal_values(splits[7], (D_INNER, RANK), D_INNER ** -0.5, 0.0625, ((0, 8),)),
        "high_down": normal_values(splits[8], (RANK, D_MODEL), RANK ** -0.5, 1.5, ((1, 32),)),
        "norm_train": jnp.clip(1.0 + 0.15 * jax.random.normal(splits[9], (D_MODEL,), jnp.float32), 0.25, 1.75),
        "norm_step": jnp.clip(jax.random.uniform(splits[10], (D_MODEL,), jnp.float32, -0.3, 0.3) * block_levels(splits[10], (D_MODEL,), ((0, 256),), -0.4, 0.0), -0.3, 0.3),
    }


mix_rate = 0.5


def reference(train_gate, low_gate, high_gate, train_up, low_up, high_up, train_down, low_down, high_down, norm_train, norm_step):
    fresh_gate = train_gate.astype(jnp.float32) + mix_rate * jnp.dot(low_gate, high_gate, preferred_element_type=jnp.float32)
    fresh_up = train_up.astype(jnp.float32) + mix_rate * jnp.dot(low_up, high_up, preferred_element_type=jnp.float32)
    fresh_down = train_down.astype(jnp.float32) + mix_rate * jnp.dot(low_down, high_down, preferred_element_type=jnp.float32)
    serve_gate = fresh_gate.T.astype(jnp.bfloat16)
    serve_up = fresh_up.T.astype(jnp.bfloat16)
    serve_down = fresh_down.T.astype(jnp.bfloat16)
    serve_norm = (norm_train + norm_step).astype(jnp.bfloat16)
    return serve_gate, serve_up, serve_down, serve_norm
```

```python
import functools

import jax
import jax.numpy as jnp
from jax import lax
from jax.experimental import pallas as pl
from jax.experimental.pallas import tpu as pltpu
from jax.sharding import Mesh
from jax.sharding import PartitionSpec as P

ZERO = ("zero_0", "zero_1")
ZERO_TP = ("zero_0", "zero_1", "tp_0", "tp_1")
TP = ("tp_0", "tp_1")
NZ, NY = 8, 4


mix_rate = 0.5

ROWS = 96
BLOCK = NY * ROWS
WIDE = 1024
CUT = 256
A_COLS = WIDE + CUT
B_COLS = WIDE + WIDE - CUT
STEP = 128

ANY = pl.BlockSpec(memory_space=pl.ANY)
VMEM = pl.BlockSpec(memory_space=pltpu.VMEM)


def shifted(x, axis, step):
    n = {"zero_0": NZ, "zero_1": NY, "tp_0": 4, "tp_1": 2}[axis]
    return lax.ppermute(x, axis, [(i, (i + step) % n) for i in range(n)])


def merged(train, low, high):
    product = lax.dot_general(
        low, high, (((0,), (0,)), ((), ())), preferred_element_type=jnp.float32
    )
    return (train.astype(jnp.float32) + mix_rate * product).astype(jnp.bfloat16)


def merge_b(td, ld, hd, tu, lu, hu, out):
    out[:, :WIDE] = merged(td[...], ld[...], hd[...])
    out[:, WIDE:] = merged(tu[:, CUT:], lu[...], hu[:, CUT:])


def merge_a(tg, lg, hg, tu, lu, hu, out):
    out[:, :WIDE] = merged(tg[...], lg[...], hg[...])
    out[:, WIDE:] = merged(tu[:, :CUT], lu[...], hu[:, :CUT])


def merge_call(body, cols, *args):
    return pl.pallas_call(
        body,
        out_shape=jax.ShapeDtypeStruct((ROWS, cols), jnp.bfloat16),
        in_specs=[VMEM] * len(args),
        out_specs=VMEM,
    )(*args)


def stack_body(starts, *refs):
    pieces, out, sems = refs[:-2], refs[-2], refs[-1]
    y = lax.axis_index("zero_1")
    copies = []
    for k, piece in enumerate(pieces):
        rel, row = starts[k]
        at = row if rel is None else lax.rem(y + rel, NY) * ROWS + row
        at = at if rel is None else pl.multiple_of(at, 16)
        copies.append(
            pltpu.make_async_copy(
                piece, out.at[pl.ds(at, piece.shape[0])], sems.at[k]
            )
        )
    for c in copies:
        c.start()
    for c in copies:
        c.wait()


def stacked(pieces, starts):
    rows = sum(p.shape[0] for p in pieces)
    nbytes = rows * pieces[0].shape[1] * 4
    return pl.pallas_call(
        functools.partial(stack_body, starts),
        out_shape=jax.ShapeDtypeStruct((rows, pieces[0].shape[1]), jnp.bfloat16),
        in_specs=[ANY] * len(pieces),
        out_specs=VMEM,
        scratch_shapes=[pltpu.SemaphoreType.DMA((len(pieces),))],
        cost_estimate=pl.CostEstimate(
            flops=nbytes * 100, bytes_accessed=nbytes, transcendentals=0
        ),
    )(*pieces)


def place_body(first, kind, blocks, nsrc, *refs):
    srcs = refs[:nsrc]
    outs = refs[nsrc + (0 if first else 3) :][:3]
    held, turned, in_sem, out_sem = refs[-4:]
    gate, up, down = outs
    z, y = lax.axis_index("zero_0"), lax.axis_index("zero_1")
    taken, loads = 0, []
    for b, (_, parts) in enumerate(blocks):
        mine = []
        for src, srow, rows, rel, row in parts:
            at = row
            if rel is not None:
                at = pl.multiple_of(lax.rem(y + rel, NY) * ROWS + row, 16)
            c = pltpu.make_async_copy(
                srcs[src].at[pl.ds(srow, rows)],
                held.at[b, pl.ds(at, rows)],
                in_sem.at[taken],
            )
            c.start()
            mine.append(c)
            taken += 1
        loads.append(mine)
    stores = []
    for b, (zrel, _) in enumerate(blocks):
        for c in loads[b]:
            c.wait()
        zabs = lax.rem(z + zrel, NZ)
        cols = pl.ds(pl.multiple_of(zabs * BLOCK, 128), BLOCK)
        if kind == "b":
            c = pltpu.make_async_copy(
                held.at[b, :, pl.ds(0, WIDE)], down.at[cols], out_sem.at[b, 0]
            )
            c.start()
            stores.append(c)
            groups = [(WIDE, WIDE - CUT, up, CUT, 1)]
        else:
            groups = [(0, WIDE, gate, 0, 0), (WIDE, CUT, up, 0, 1)]
        for start, width, out, row, k in groups:
            base = start if kind == "a" else start - WIDE

            def turn(i, _, start=start, base=base, b=b):
                src = pl.multiple_of(start + i * STEP, STEP)
                dst = pl.multiple_of(base + i * STEP, STEP)
                turned[b, pl.ds(dst, STEP), :] = held[b, :, pl.ds(src, STEP)].T
                return 0

            lax.fori_loop(0, width // STEP, turn, 0)
            c = pltpu.make_async_copy(
                turned.at[b, pl.ds(base, width)],
                out.at[pl.ds(row, width), cols],
                out_sem.at[b, k],
            )
            c.start()
            stores.append(c)
    for c in stores:
        c.wait()


OUT_SHAPES = (
    jax.ShapeDtypeStruct((WIDE, NZ * BLOCK), jnp.bfloat16),
    jax.ShapeDtypeStruct((WIDE, NZ * BLOCK), jnp.bfloat16),
    jax.ShapeDtypeStruct((NZ * BLOCK, WIDE), jnp.bfloat16),
)


def placed(outs, kind, blocks, srcs):
    first = outs is None
    n = len(blocks)
    cols = A_COLS if kind == "a" else B_COLS
    tall = A_COLS if kind == "a" else WIDE - CUT
    extra = () if first else tuple(outs)
    nbytes = n * BLOCK * cols * 4
    return pl.pallas_call(
        functools.partial(place_body, first, kind, blocks, len(srcs)),
        out_shape=OUT_SHAPES,
        in_specs=[ANY] * (len(srcs) + len(extra)),
        out_specs=[ANY] * 3,
        input_output_aliases={}
        if first
        else {len(srcs) + k: k for k in range(3)},
        scratch_shapes=[
            pltpu.VMEM((n, BLOCK, cols), jnp.bfloat16),
            pltpu.VMEM((n, tall, BLOCK), jnp.bfloat16),
            pltpu.SemaphoreType.DMA((sum(len(b[1]) for b in blocks),)),
            pltpu.SemaphoreType.DMA((n, 2)),
        ],
        cost_estimate=pl.CostEstimate(
            flops=nbytes * 200, bytes_accessed=nbytes, transcendentals=0
        ),
    )(*srcs, *extra)


def per_device(
    train_gate,
    low_gate,
    high_gate,
    train_up,
    low_up,
    high_up,
    train_down,
    low_down,
    high_down,
    norm_train,
    norm_step,
):
    z, y = "zero_0", "zero_1"
    own_b = merge_call(
        merge_b, B_COLS, train_down.T, high_down, low_down.T, train_up, low_up.T, high_up
    )
    own_a = merge_call(
        merge_a, A_COLS, train_gate, low_gate.T, high_gate, train_up, low_up.T, high_up
    )
    half = ROWS // 2
    a_l, a_r = shifted(own_a, y, 1), shifted(own_a, y, -1)
    a_top, a_low = shifted(a_l[:half], y, 1), shifted(a_r[half:], y, -1)
    block = stacked(
        (own_a, a_l, a_r, a_top, a_low), ((0, 0), (3, 0), (1, 0), (2, 0), (2, half))
    )
    f1, g1 = shifted(own_b, z, 1), shifted(own_b, z, -1)
    f2, g2 = shifted(f1, z, 1), shifted(g1, z, -1)
    f3, g3 = shifted(f2, z, 1), shifted(g2, z, -1)
    f4, g4 = shifted(f3[:half], z, 1), shifted(g3[half:], z, -1)
    groups = [
        (own_b, (0,)),
        (stacked((f1, g1), ((None, 0), (None, 96))), (7, 1)),
        (stacked((f2, g2), ((None, 0), (None, 96))), (6, 2)),
        (
            stacked(
                (f3, g3, f4, g4), ((None, 0), (None, 96), (None, 192), (None, 240))
            ),
            (5, 3, 4),
        ),
    ]
    p1, q1 = shifted(block, z, 1), shifted(block, z, -1)
    p2, q2 = shifted(p1, z, 1), shifted(q1, z, -1)
    p3, q3 = shifted(p2, z, 1), shifted(q2, z, -1)
    mid = BLOCK // 2
    p4, q4 = shifted(p3[:mid], z, 1), shifted(q3[mid:], z, -1)
    whole = []
    for k, (group, rels) in enumerate(groups):
        left, right = shifted(group, y, 1), shifted(group, y, -1)
        far = shifted(left, y, 1) if k in (0, 3) else shifted(right, y, -1)
        whole.append(((group, left, right, far), rels))

    def b_blocks(rels):
        return tuple(
            (
                rel,
                tuple((s, i * ROWS, ROWS, yrel, 0) for s, yrel in enumerate((0, 3, 1, 2))),
            )
            for i, rel in enumerate(rels)
        )

    def a_block(rel, s):
        return (rel, ((s, 0, BLOCK, None, 0),))

    outs = placed(None, "a", (a_block(0, 0),), (block,))
    outs = placed(outs, "a", (a_block(7, 0), a_block(1, 1)), (p1, q1))
    outs = placed(outs, "b", b_blocks(whole[0][1]), whole[0][0])
    outs = placed(outs, "a", (a_block(6, 0), a_block(2, 1)), (p2, q2))
    outs = placed(outs, "b", b_blocks(whole[1][1]), whole[1][0])
    outs = placed(outs, "a", (a_block(5, 0), a_block(3, 1)), (p3, q3))
    outs = placed(outs, "b", b_blocks(whole[2][1]), whole[2][0])
    outs = placed(
        outs, "a", ((4, ((0, 0, mid, None, 0), (1, 0, mid, None, mid))),), (p4, q4)
    )
    outs = placed(outs, "b", b_blocks(whole[3][1]), whole[3][0])

    gain = (norm_train + norm_step).astype(jnp.bfloat16)
    place = lax.axis_index(ZERO_TP) * gain.shape[0]
    full = lax.dynamic_update_slice(
        jnp.zeros((gain.shape[0] * 256,), jnp.bfloat16), gain, (place,)
    )
    for axis, step in (
        ("tp_1", 1),
        ("tp_0", 1),
        ("tp_0", 2),
        (y, 1),
        (y, 2),
        (z, 1),
        (z, 2),
        (z, 4),
    ):
        full = full + shifted(full, axis, step)
    return (*outs, full)


def solution(mesh):
    finer = Mesh(mesh.devices.reshape(8, 4, 4, 2), ("zero_0", "zero_1", "tp_0", "tp_1"))
    in_specs = (
        P(ZERO, TP),
        P(ZERO, None),
        P(None, TP),
        P(ZERO, TP),
        P(ZERO, None),
        P(None, TP),
        P(TP, ZERO),
        P(TP, None),
        P(None, ZERO),
        P(ZERO_TP),
        P(ZERO_TP),
    )
    out_specs = (P(TP, None), P(TP, None), P(None, TP), P())
    return jax.shard_map(
        per_device, mesh=finer, in_specs=in_specs, out_specs=out_specs, check_vma=False
    )
```

```python
import functools

import jax
import jax.numpy as jnp
from jax import lax
from jax.experimental import pallas as pl
from jax.experimental.pallas import tpu as pltpu
from jax.sharding import Mesh
from jax.sharding import PartitionSpec as P


ZERO = ("zero_0", "zero_1")
ZERO_TP = ("zero_0", "zero_1", "tp_0", "tp_1")
TP = ("tp_0", "tp_1")
NZ, NY = 8, 4
D_MODEL, D_INNER, RANK = 3072, 8192, 16


mix_rate = 0.5

ROWS = 96
BLOCK = NY * ROWS
WIDE = 1024
CUT = 128
A_COLS = WIDE + CUT
B_COLS = WIDE + WIDE - CUT
STEP = 128

ANY = pl.BlockSpec(memory_space=pl.ANY)
VMEM = pl.BlockSpec(memory_space=pltpu.VMEM)


def shifted(x, axis, step):
    n = {"zero_0": NZ, "zero_1": NY, "tp_0": 4, "tp_1": 2}[axis]
    return lax.ppermute(x, axis, [(i, (i + step) % n) for i in range(n)])


def merged(train, low, high):
    product = lax.dot_general(
        low, high, (((0,), (0,)), ((), ())), preferred_element_type=jnp.float32
    )
    return (train.astype(jnp.float32) + mix_rate * product).astype(jnp.bfloat16)


def merge_body(tg, lg, hg, td, ld, hd, tu, lu, hu, out_a, out_b):
    up = merged(tu[...], lu[...], hu[...])
    out_a[:, :WIDE] = merged(tg[...], lg[...], hg[...])
    out_a[:, WIDE:] = up[:, :CUT]
    out_b[:, :WIDE] = merged(td[...], ld[...], hd[...])
    out_b[:, WIDE:] = up[:, CUT:]


def merge_call(*args):
    return pl.pallas_call(
        merge_body,
        out_shape=(
            jax.ShapeDtypeStruct((ROWS, A_COLS), jnp.bfloat16),
            jax.ShapeDtypeStruct((ROWS, B_COLS), jnp.bfloat16),
        ),
        in_specs=[VMEM] * len(args),
        out_specs=(VMEM, VMEM),
    )(*args)


def stack_body(starts, *refs):
    pieces, out, sems = refs[:-2], refs[-2], refs[-1]
    y = lax.axis_index("zero_1")
    copies = []
    for k, piece in enumerate(pieces):
        rel, row = starts[k]
        at = row if rel is None else lax.rem(y + rel, NY) * ROWS + row
        at = at if rel is None else pl.multiple_of(at, 16)
        copies.append(
            pltpu.make_async_copy(
                piece, out.at[pl.ds(at, piece.shape[0])], sems.at[k]
            )
        )
    for c in copies:
        c.start()
    for c in copies:
        c.wait()


def stacked(pieces, starts):
    rows = sum(p.shape[0] for p in pieces)
    nbytes = rows * pieces[0].shape[1] * 4
    return pl.pallas_call(
        functools.partial(stack_body, starts),
        out_shape=jax.ShapeDtypeStruct((rows, pieces[0].shape[1]), jnp.bfloat16),
        in_specs=[ANY] * len(pieces),
        out_specs=VMEM,
        scratch_shapes=[pltpu.SemaphoreType.DMA((len(pieces),))],
        cost_estimate=pl.CostEstimate(
            flops=nbytes * 100, bytes_accessed=nbytes, transcendentals=0
        ),
    )(*pieces)


def place_body(first, kind, blocks, nsrc, *refs):
    srcs = refs[:nsrc]
    outs = refs[nsrc + (0 if first else 3) :][:3]
    held, turned, in_sem, out_sem = refs[-4:]
    gate, up, down = outs
    z, y = lax.axis_index("zero_0"), lax.axis_index("zero_1")
    taken, loads = 0, []
    for b, (_, parts) in enumerate(blocks):
        mine = []
        for src, srow, rows, rel, row in parts:
            at = row
            if rel is not None:
                at = pl.multiple_of(lax.rem(y + rel, NY) * ROWS + row, 16)
            c = pltpu.make_async_copy(
                srcs[src].at[pl.ds(srow, rows)],
                held.at[b, pl.ds(at, rows)],
                in_sem.at[taken],
            )
            c.start()
            mine.append(c)
            taken += 1
        loads.append(mine)
    stores = []
    for b, (zrel, _) in enumerate(blocks):
        for c in loads[b]:
            c.wait()
        zabs = lax.rem(z + zrel, NZ)
        cols = pl.ds(pl.multiple_of(zabs * BLOCK, 128), BLOCK)
        if kind == "b":
            c = pltpu.make_async_copy(
                held.at[b, :, pl.ds(0, WIDE)], down.at[cols], out_sem.at[b, 0]
            )
            c.start()
            stores.append(c)
            groups = [(WIDE, WIDE - CUT, up, CUT, 1)]
        else:
            groups = [(0, WIDE, gate, 0, 0), (WIDE, CUT, up, 0, 1)]
        for start, width, out, row, k in groups:
            base = start if kind == "a" else start - WIDE

            def turn(i, _, start=start, base=base, b=b):
                src = pl.multiple_of(start + i * STEP, STEP)
                dst = pl.multiple_of(base + i * STEP, STEP)
                turned[b, pl.ds(dst, STEP), :] = held[b, :, pl.ds(src, STEP)].T
                return 0

            lax.fori_loop(0, width // STEP, turn, 0)
            c = pltpu.make_async_copy(
                turned.at[b, pl.ds(base, width)],
                out.at[pl.ds(row, width), cols],
                out_sem.at[b, k],
            )
            c.start()
            stores.append(c)
    for c in stores:
        c.wait()


OUT_SHAPES = (
    jax.ShapeDtypeStruct((WIDE, NZ * BLOCK), jnp.bfloat16),
    jax.ShapeDtypeStruct((WIDE, NZ * BLOCK), jnp.bfloat16),
    jax.ShapeDtypeStruct((NZ * BLOCK, WIDE), jnp.bfloat16),
)


def placed(outs, kind, blocks, srcs):
    first = outs is None
    n = len(blocks)
    cols = A_COLS if kind == "a" else B_COLS
    tall = A_COLS if kind == "a" else WIDE - CUT
    extra = () if first else tuple(outs)
    nbytes = n * BLOCK * cols * 4
    return pl.pallas_call(
        functools.partial(place_body, first, kind, blocks, len(srcs)),
        out_shape=OUT_SHAPES,
        in_specs=[ANY] * (len(srcs) + len(extra)),
        out_specs=[ANY] * 3,
        input_output_aliases={}
        if first
        else {len(srcs) + k: k for k in range(3)},
        scratch_shapes=[
            pltpu.VMEM((n, BLOCK, cols), jnp.bfloat16),
            pltpu.VMEM((n, tall, BLOCK), jnp.bfloat16),
            pltpu.SemaphoreType.DMA((sum(len(b[1]) for b in blocks),)),
            pltpu.SemaphoreType.DMA((n, 2)),
        ],
        cost_estimate=pl.CostEstimate(
            flops=nbytes * 200, bytes_accessed=nbytes, transcendentals=0
        ),
    )(*srcs, *extra)


def per_device(
    train_gate,
    low_gate,
    high_gate,
    train_up,
    low_up,
    high_up,
    train_down,
    low_down,
    high_down,
    norm_train,
    norm_step,
):
    z, y = "zero_0", "zero_1"
    half, mid, part = ROWS // 2, BLOCK // 2, 3 * ROWS // 2

    gain = (norm_train + norm_step).astype(jnp.bfloat16)
    place = lax.axis_index(ZERO_TP) * gain.shape[0]
    full = lax.dynamic_update_slice(
        jnp.zeros((gain.shape[0] * 256,), jnp.bfloat16), gain, (place,)
    )

    def doubled(full, axis, step):
        return full + shifted(full, axis, step)

    def b_blocks(rels):
        return tuple(
            (
                rel,
                tuple(
                    (s, i * ROWS, ROWS, yrel, 0) for s, yrel in enumerate((0, 3, 1, 2))
                ),
            )
            for i, rel in enumerate(rels)
        )

    def a_block(rel, s):
        return (rel, ((s, 0, BLOCK, None, 0),))

    own_a, own_b = merge_call(
        train_gate,
        low_gate.T,
        high_gate,
        train_down.T,
        high_down,
        low_down.T,
        train_up,
        low_up.T,
        high_up,
    )
    a_l = shifted(own_a, y, 1)
    a_r = shifted(own_a, y, -1)
    f1 = shifted(own_b, z, 1)
    g1 = shifted(own_b, z, -1)
    l0 = shifted(own_b, y, 1)
    full = doubled(full, "tp_1", 1)
    a_f = shifted(a_r, y, -1)
    r0 = shifted(own_b, y, -1)
    f2 = shifted(f1, z, 1)
    g2 = shifted(g1, z, -1)
    s1 = stacked((f1, g1), ((None, 0), (None, 96)))
    l1 = shifted(s1, y, 1)
    r1 = shifted(s1, y, -1)
    block = stacked((own_a, a_l, a_r, a_f), ((0, 0), (3, 0), (1, 0), (2, 0)))
    p1 = shifted(block, z, 1)
    q1 = shifted(block, z, -1)
    o0 = shifted(l0, y, 1)
    full = doubled(full, "tp_0", 1)
    f3 = shifted(f2, z, 1)
    g3 = shifted(g2, z, -1)
    s2 = stacked((f2, g2), ((None, 0), (None, 96)))
    l2 = shifted(s2, y, 1)
    r2 = shifted(s2, y, -1)
    full = doubled(full, "tp_0", 2)
    outs = placed(None, "a", (a_block(0, 0),), (block,))
    o1 = shifted(r1, y, -1)
    full = doubled(full, y, 1)
    outs = placed(outs, "b", b_blocks((0,)), (own_b, l0, r0, o0))
    f4 = shifted(f3[:half], z, 1)
    g4 = shifted(g3[half:], z, -1)
    p2 = shifted(p1, z, 1)
    q2 = shifted(q1, z, -1)
    full = doubled(full, y, 2)
    outs = placed(outs, "a", (a_block(7, 0), a_block(1, 1)), (p1, q1))
    o2 = shifted(l2, y, 1)
    s3 = stacked((f3, g3, f4, g4), ((None, 0), (None, 96), (None, 192), (None, 240)))
    l3 = shifted(s3, y, 1)
    r3 = shifted(s3, y, -1)
    full = doubled(full, z, 1)
    outs = placed(outs, "b", b_blocks((7, 1)), (s1, l1, r1, o1))
    p3 = shifted(p2, z, 1)
    q3 = shifted(q2, z, -1)
    full = doubled(full, z, 2)
    outs = placed(outs, "a", (a_block(6, 0), a_block(2, 1)), (p2, q2))
    outs = placed(outs, "b", b_blocks((6, 2)), (s2, l2, r2, o2))
    full = doubled(full, z, 4)
    t3 = shifted(l3[:part], y, 1)
    b3 = shifted(r3[part:], y, -1)
    p4 = shifted(p3[:mid], z, 1)
    q4 = shifted(q3[mid:], z, -1)
    outs = placed(outs, "a", (a_block(5, 0), a_block(3, 1)), (p3, q3))
    near = [[(s, i * ROWS, ROWS, r, 0) for s, r in enumerate((0, 3, 1))] for i in range(3)]
    far = (
        [(3, 0, ROWS, 2, 0)],
        [(3, ROWS, half, 2, 0), (4, 0, half, 2, half)],
        [(4, half, ROWS, 2, 0)],
    )
    outs = placed(
        outs,
        "b",
        tuple(
            (rel, tuple(n + f)) for rel, n, f in zip((5, 3, 4), near, far, strict=True)
        ),
        (s3, l3, r3, t3, b3),
    )
    outs = placed(
        outs, "a", ((4, ((0, 0, mid, None, 0), (1, 0, mid, None, mid))),), (p4, q4)
    )
    return (*outs, full)


def solution(mesh):
    finer = Mesh(mesh.devices.reshape(8, 4, 4, 2), ("zero_0", "zero_1", "tp_0", "tp_1"))
    in_specs = (
        P(ZERO, TP),
        P(ZERO, None),
        P(None, TP),
        P(ZERO, TP),
        P(ZERO, None),
        P(None, TP),
        P(TP, ZERO),
        P(TP, None),
        P(None, ZERO),
        P(ZERO_TP),
        P(ZERO_TP),
    )
    out_specs = (P(TP, None), P(TP, None), P(None, TP), P())

    step = jax.shard_map(
        per_device, mesh=finer, in_specs=in_specs, out_specs=out_specs, check_vma=False
    )
    low, wide = D_MODEL, D_INNER
    shapes = ((low, wide), (low, RANK), (RANK, wide)) * 2
    shapes += ((wide, low), (wide, RANK), (RANK, low))
    jax.eval_shape(
        step,
        *(jax.ShapeDtypeStruct(s, jnp.bfloat16) for s in shapes),
        *(jax.ShapeDtypeStruct((low,), jnp.float32) for _ in range(2)),
    )
    return step
```

```python
import functools

import jax
import jax.numpy as jnp
from jax import lax
from jax.experimental import pallas as pl
from jax.experimental.pallas import tpu as pltpu
from jax.sharding import Mesh
from jax.sharding import PartitionSpec as P


ZERO = ("zero_0", "zero_1")
ZERO_TP = ("zero_0", "zero_1", "tp_0", "tp_1")
TP = ("tp_0", "tp_1")
NZ, NY = 8, 4
D_MODEL, D_INNER, RANK = 3072, 8192, 16


mix_rate = 0.5

ROWS = 96
BLOCK = NY * ROWS
WIDE = 1024
CUT = 128
A_COLS = WIDE + CUT
B_COLS = WIDE + WIDE - CUT
STEP = 128
UP = 192
GRANT = 1 << 20

ANY = pl.BlockSpec(memory_space=pl.ANY)
VMEM = pl.BlockSpec(memory_space=pltpu.VMEM)
HBM = pl.BlockSpec(memory_space=pltpu.HBM)


SIZES = {"zero_0": NZ, "zero_1": NY, "tp_0": 4, "tp_1": 2}


def shifted(x, axis, step):
    n = SIZES[axis]
    return lax.ppermute(x, axis, [(i, (i + step) % n) for i in range(n)])


def merged(train, low, high):
    product = lax.dot_general(
        low, high, (((0,), (0,)), ((), ())), preferred_element_type=jnp.float32
    )
    return (train.astype(jnp.float32) + mix_rate * product).astype(jnp.bfloat16)


def merge_body(*refs):
    ins, (out_all, out_b), held, sems = refs[:9], refs[9:11], refs[11:20], refs[20]
    loads = [
        pltpu.make_async_copy(src, dst, sems.at[k])
        for k, (src, dst) in enumerate(zip(ins, held, strict=True))
    ]
    for c in loads:
        c.start()
    for c in loads:
        c.wait()
    tg, lg, hg, td, ld, hd, tu, lu, hu = held
    up = merged(tu[...], lu[...], hu[...])
    down = merged(td[...], ld[...], hd[...])
    for out, at in ((out_b, 0), (out_all, A_COLS)):
        out[:, at : at + WIDE] = down
        out[:, at + WIDE : at + B_COLS] = up[:, CUT:]
    out_all[:, :WIDE] = merged(tg[...], lg[...], hg[...])
    if CUT:
        out_all[:, WIDE:A_COLS] = up[:, :CUT]


def merge_call(*args):
    return pl.pallas_call(
        merge_body,
        out_shape=(
            jax.ShapeDtypeStruct((ROWS, A_COLS + B_COLS), jnp.bfloat16),
            jax.ShapeDtypeStruct((ROWS, B_COLS), jnp.bfloat16),
        ),
        in_specs=[HBM] * len(args),
        out_specs=(VMEM, VMEM),
        scratch_shapes=[pltpu.VMEM(a.shape, a.dtype) for a in args]
        + [pltpu.SemaphoreType.DMA((len(args),))],
    )(*args)


def stack_body(starts, *refs):
    pieces, out, sems = refs[:-2], refs[-2], refs[-1]
    y = lax.axis_index("zero_1")
    copies = []
    for k, piece in enumerate(pieces):
        rel, row = starts[k]
        at = row if rel is None else lax.rem(y + rel, NY) * ROWS + row
        at = at if rel is None else pl.multiple_of(at, 16)
        copies.append(
            pltpu.make_async_copy(
                piece.at[:, pl.ds(0, out.shape[1])],
                out.at[pl.ds(at, piece.shape[0])],
                sems.at[k],
            )
        )
    for c in copies:
        c.start()
    for c in copies:
        c.wait()


def stacked(pieces, starts, cols=B_COLS):
    rows = sum(p.shape[0] for p in pieces)
    nbytes = rows * cols * 4
    return pl.pallas_call(
        functools.partial(stack_body, starts),
        out_shape=jax.ShapeDtypeStruct((rows, cols), jnp.bfloat16),
        in_specs=[ANY] * len(pieces),
        out_specs=VMEM,
        scratch_shapes=[pltpu.SemaphoreType.DMA((len(pieces),))],
        compiler_params=pltpu.CompilerParams(vmem_limit_bytes=nbytes + GRANT),
        cost_estimate=pl.CostEstimate(
            flops=nbytes * 100, bytes_accessed=nbytes, transcendentals=0
        ),
    )(*pieces)


def place_body(first, blocks, nsrc, *refs):
    srcs = refs[:nsrc]
    outs = refs[nsrc + (0 if first else 3) :][:3]
    held, turned, in_sem, out_sem = refs[-4:]
    gate, up, down = outs
    z, y = lax.axis_index("zero_0"), lax.axis_index("zero_1")
    taken, loads = 0, []
    for b, (kind, _, parts) in enumerate(blocks):
        mine = []
        cols = pl.ds(0, A_COLS if kind == "a" else B_COLS)
        for src, srow, rows, rel, row in parts:
            at = row
            if rel is not None:
                at = pl.multiple_of(lax.rem(y + rel, NY) * ROWS + row, 16)
            c = pltpu.make_async_copy(
                srcs[src].at[
                    pl.ds(srow, rows), pl.ds(srcs[src].shape[1] - cols.size, cols.size)
                ],
                held.at[b, pl.ds(at, rows), cols],
                in_sem.at[taken],
            )
            c.start()
            mine.append(c)
            taken += 1
        loads.append(mine)
    stores = []
    for b, (kind, zrel, _) in enumerate(blocks):
        for c in loads[b]:
            c.wait()
        zabs = lax.rem(z + zrel, NZ)
        cols = pl.ds(pl.multiple_of(zabs * BLOCK, 128), BLOCK)
        if kind == "b":
            c = pltpu.make_async_copy(
                held.at[b, :, pl.ds(0, WIDE)], down.at[cols], out_sem.at[b, 0]
            )
            c.start()
            stores.append(c)
            groups = [(WIDE, WIDE - CUT, up, CUT, 1)]
        else:
            groups = [(0, WIDE, gate, 0, 0)]
            groups += [(WIDE, CUT, up, 0, 1)] if CUT else []
        for start, width, out, row, k in groups:
            base = start if kind == "a" else start - WIDE

            def turn(i, _, start=start, base=base, b=b):
                src = pl.multiple_of(start + i * STEP, STEP)
                dst = pl.multiple_of(base + i * STEP, STEP)
                turned[b, pl.ds(dst, STEP), :] = held[b, :, pl.ds(src, STEP)].T
                return 0

            lax.fori_loop(0, width // STEP, turn, 0)
            c = pltpu.make_async_copy(
                turned.at[b, pl.ds(base, width)],
                out.at[pl.ds(row, width), cols],
                out_sem.at[b, k],
            )
            c.start()
            stores.append(c)
    for c in stores:
        c.wait()


OUT_SHAPES = (
    jax.ShapeDtypeStruct((WIDE, NZ * BLOCK), jnp.bfloat16),
    jax.ShapeDtypeStruct((WIDE, NZ * BLOCK), jnp.bfloat16),
    jax.ShapeDtypeStruct((NZ * BLOCK, WIDE), jnp.bfloat16),
)


def placed(outs, blocks, srcs):
    first = outs is None
    n = len(blocks)
    kinds = {b[0] for b in blocks}
    cols = B_COLS if "b" in kinds else A_COLS
    tall = A_COLS if "a" in kinds else WIDE - CUT
    extra = () if first else tuple(outs)
    nbytes = n * BLOCK * cols * 4
    grant = 2 * n * BLOCK * (cols + tall) + GRANT
    return pl.pallas_call(
        functools.partial(place_body, first, blocks, len(srcs)),
        out_shape=OUT_SHAPES,
        in_specs=[ANY] * len(srcs) + [HBM] * len(extra),
        out_specs=[HBM] * 3,
        input_output_aliases={}
        if first
        else {len(srcs) + k: k for k in range(3)},
        scratch_shapes=[
            pltpu.VMEM((n, BLOCK, cols), jnp.bfloat16),
            pltpu.VMEM((n, tall, BLOCK), jnp.bfloat16),
            pltpu.SemaphoreType.DMA((sum(len(b[2]) for b in blocks),)),
            pltpu.SemaphoreType.DMA((n, 2)),
        ],
        compiler_params=pltpu.CompilerParams(vmem_limit_bytes=grant),
        cost_estimate=pl.CostEstimate(
            flops=nbytes * 200, bytes_accessed=nbytes, transcendentals=0
        ),
    )(*srcs, *extra)


def per_device(
    train_gate,
    low_gate,
    high_gate,
    train_up,
    low_up,
    high_up,
    train_down,
    low_down,
    high_down,
    norm_train,
    norm_step,
):
    z, y = "zero_0", "zero_1"
    part = 112

    gain = (norm_train + norm_step).astype(jnp.bfloat16)
    place = lax.axis_index(ZERO_TP) * gain.shape[0]
    full = lax.dynamic_update_slice(
        jnp.zeros((gain.shape[0] * 256,), jnp.bfloat16), gain, (place,)
    )
    full = lax.optimization_barrier(full)

    def sent(k, full):
        axis, step = (
            (z, -1),
            (y, -1),
            (y, 2),
            ("tp_1", 1),
            ("tp_0", 1),
            (z, -2),
            ("tp_0", 2),
            (z, 4),
        )[k]
        return shifted(full, axis, step)

    def added(full, other):
        return full + other

    def b_blocks(rels, at):
        return tuple(
            (
                "b",
                rel,
                tuple(
                    (at + s, i * ROWS, ROWS, yrel, 0)
                    for s, yrel in enumerate((0, 3, 1, 2))
                ),
            )
            for i, rel in enumerate(rels)
        )

    def a_block(rel, s):
        return ("a", rel, ((s, 0, BLOCK, None, 0),))

    own, own_b = merge_call(
        train_gate,
        low_gate.T,
        high_gate,
        train_down.T,
        high_down,
        low_down.T,
        train_up,
        low_up.T,
        high_up,
    )
    l0 = shifted(own, y, 1)
    r0 = shifted(own, y, -1)
    f1 = shifted(own_b, z, 1)
    g1 = shifted(own_b, z, -1)
    o0 = shifted(l0, y, 1)
    f2 = shifted(f1, z, 1)
    g2 = shifted(g1, z, -1)
    s1 = stacked((f1, g1), ((None, 0), (None, 96)))
    r1 = shifted(s1, y, -1)
    l1 = shifted(s1, y, 1)
    n0 = sent(0, full)
    f3 = shifted(f2, z, 1)
    g3 = shifted(g2, z, -1)
    block = stacked((own, l0, r0, o0), ((0, 0), (3, 0), (1, 0), (2, 0)), A_COLS)
    p1 = shifted(block, z, 1)
    q1 = shifted(block, z, -1)
    s2 = stacked((f2, g2), ((None, 0), (None, 96)))
    full = added(full, n0)
    n1 = sent(1, full)
    r2 = shifted(s2, y, -1)
    l2 = shifted(s2, y, 1)
    outs = placed(None, (a_block(0, 0),), (block,))
    outs = placed(outs, b_blocks((0,), 0), (own, l0, r0, o0))
    f4 = shifted(f3, z, 1)
    full = added(full, n1)
    n2 = sent(2, full)
    o1 = shifted(l1, y, 1)
    o2 = shifted(r2, y, -1)
    q2 = shifted(q1, z, -1)
    p2 = shifted(p1, z, 1)
    full = added(full, n2)
    n3 = sent(3, full)
    s3 = stacked((f3, g3, f4), ((None, 0), (None, 96), (None, 192)))
    l3 = shifted(s3, y, 1)
    r3 = shifted(s3, y, -1)
    full = added(full, n3)
    n4 = sent(4, full)
    outs = placed(outs, (a_block(7, 0), a_block(1, 1)), (p1, q1))
    full = added(full, n4)
    n5 = sent(5, full)
    q3 = shifted(q2, z, -1)
    p3 = shifted(p2, z, 1)
    outs = placed(outs, b_blocks((7, 1), 0), (s1, l1, r1, o1))
    full = added(full, n5)
    n6 = sent(6, full)
    outs = placed(outs, b_blocks((6, 2), 0), (s2, l2, r2, o2))
    outs = placed(outs, (a_block(6, 0), a_block(2, 1)), (p2, q2))
    b3 = shifted(r3[part:], y, -1)
    t3 = shifted(l3[:part], y, 1)
    q4 = shifted(q3[UP:], z, -1)
    p4 = shifted(p3[:UP], z, 1)
    full = added(full, n6)
    n7 = sent(7, full)
    outs = placed(outs, (a_block(5, 0), a_block(3, 1)), (p3, q3))
    near = [[(s, i * ROWS, ROWS, r, 0) for s, r in enumerate((0, 3, 1))] for i in range(3)]
    cut = part - ROWS
    far = (
        ((3, 0, ROWS, 2, 0),),
        ((3, ROWS, cut, 2, 0), (4, 0, ROWS - cut, 2, cut)),
        ((4, ROWS - cut, ROWS, 2, 0),),
    )
    outs = placed(
        outs,
        tuple(
            ("b", rel, (*n, *f)) for rel, n, f in zip((5, 3, 4), near, far, strict=True)
        ),
        (s3, l3, r3, t3, b3),
    )
    outs = placed(
        outs, (("a", 4, ((0, 0, UP, None, 0), (1, 0, BLOCK - UP, None, UP))),), (p4, q4)
    )
    full = added(full, n7)
    return (*outs, full)


def solution(mesh):
    finer = Mesh(mesh.devices.reshape(8, 4, 4, 2), ("zero_0", "zero_1", "tp_0", "tp_1"))
    in_specs = (
        P(ZERO, TP),
        P(ZERO, None),
        P(None, TP),
        P(ZERO, TP),
        P(ZERO, None),
        P(None, TP),
        P(TP, ZERO),
        P(TP, None),
        P(None, ZERO),
        P(ZERO_TP),
        P(ZERO_TP),
    )
    out_specs = (P(TP, None), P(TP, None), P(None, TP), P())

    step = jax.shard_map(
        per_device, mesh=finer, in_specs=in_specs, out_specs=out_specs, check_vma=False
    )
    low, wide = D_MODEL, D_INNER
    shapes = ((low, wide), (low, RANK), (RANK, wide)) * 2
    shapes += ((wide, low), (wide, RANK), (RANK, low))
    jax.eval_shape(
        step,
        *(jax.ShapeDtypeStruct(s, jnp.bfloat16) for s in shapes),
        *(jax.ShapeDtypeStruct((low,), jnp.float32) for _ in range(2)),
    )
    return step
```

```python
import functools

import jax
import jax.numpy as jnp
from jax import lax
from jax.experimental import pallas as pl
from jax.experimental.pallas import tpu as pltpu
from jax.sharding import Mesh
from jax.sharding import PartitionSpec as P


ZERO = ("zero_0", "zero_1")
ZERO_TP = ("zero_0", "zero_1", "tp_0", "tp_1")
TP = ("tp_0", "tp_1")
NZ, NY = 8, 4
D_MODEL, D_INNER, RANK = 3072, 8192, 16


mix_rate = 0.5

ROWS = 96
BLOCK = NY * ROWS
WIDE = 1024
CUT = 128
A_COLS = WIDE + CUT
B_COLS = WIDE + WIDE - CUT
STEP = 128
UP = 160
GRANT = 1 << 20

ANY = pl.BlockSpec(memory_space=pl.ANY)
VMEM = pl.BlockSpec(memory_space=pltpu.VMEM)
HBM = pl.BlockSpec(memory_space=pltpu.HBM)


SIZES = {"zero_0": NZ, "zero_1": NY, "tp_0": 4, "tp_1": 2}


def shifted(x, axis, step):
    n = SIZES[axis]
    return lax.ppermute(x, axis, [(i, (i + step) % n) for i in range(n)])


def merged(train, low, high):
    product = lax.dot_general(
        low, high, (((0,), (0,)), ((), ())), preferred_element_type=jnp.float32
    )
    return (train.astype(jnp.float32) + mix_rate * product).astype(jnp.bfloat16)


def merge_body(*refs):
    ins, (out_all, out_b), held, sems = refs[:9], refs[9:11], refs[11:20], refs[20]
    loads = [
        pltpu.make_async_copy(src, dst, sems.at[k])
        for k, (src, dst) in enumerate(zip(ins, held, strict=True))
    ]
    for c in loads:
        c.start()
    for c in loads:
        c.wait()
    tg, lg, hg, td, ld, hd, tu, lu, hu = held
    up = merged(tu[...], lu[...], hu[...])
    down = merged(td[...], ld[...], hd[...])
    for out, at in ((out_b, 0), (out_all, A_COLS)):
        out[:, at : at + WIDE] = down
        out[:, at + WIDE : at + B_COLS] = up[:, CUT:]
    out_all[:, :WIDE] = merged(tg[...], lg[...], hg[...])
    if CUT:
        out_all[:, WIDE:A_COLS] = up[:, :CUT]


def merge_call(*args):
    return pl.pallas_call(
        merge_body,
        out_shape=(
            jax.ShapeDtypeStruct((ROWS, A_COLS + B_COLS), jnp.bfloat16),
            jax.ShapeDtypeStruct((ROWS, B_COLS), jnp.bfloat16),
        ),
        in_specs=[HBM] * len(args),
        out_specs=(VMEM, VMEM),
        scratch_shapes=[pltpu.VMEM(a.shape, a.dtype) for a in args]
        + [pltpu.SemaphoreType.DMA((len(args),))],
    )(*args)


def stack_body(starts, *refs):
    pieces, out, sems = refs[:-2], refs[-2], refs[-1]
    y = lax.axis_index("zero_1")
    copies = []
    for k, piece in enumerate(pieces):
        rel, row = starts[k]
        at = row if rel is None else lax.rem(y + rel, NY) * ROWS + row
        at = at if rel is None else pl.multiple_of(at, 16)
        copies.append(
            pltpu.make_async_copy(
                piece.at[:, pl.ds(0, out.shape[1])],
                out.at[pl.ds(at, piece.shape[0])],
                sems.at[k],
            )
        )
    for c in copies:
        c.start()
    for c in copies:
        c.wait()


def stacked(pieces, starts, cols=B_COLS):
    rows = sum(p.shape[0] for p in pieces)
    nbytes = rows * cols * 4
    return pl.pallas_call(
        functools.partial(stack_body, starts),
        out_shape=jax.ShapeDtypeStruct((rows, cols), jnp.bfloat16),
        in_specs=[ANY] * len(pieces),
        out_specs=VMEM,
        scratch_shapes=[pltpu.SemaphoreType.DMA((len(pieces),))],
        compiler_params=pltpu.CompilerParams(vmem_limit_bytes=nbytes + GRANT),
        cost_estimate=pl.CostEstimate(
            flops=nbytes * 100, bytes_accessed=nbytes, transcendentals=0
        ),
    )(*pieces)


def place_body(first, blocks, nsrc, *refs):
    srcs = refs[:nsrc]
    outs = refs[nsrc + (0 if first else 3) :][:3]
    held, turned, in_sem, out_sem = refs[-4:]
    gate, up, down = outs
    z, y = lax.axis_index("zero_0"), lax.axis_index("zero_1")
    taken, loads = 0, []
    for b, (kind, _, parts) in enumerate(blocks):
        mine = []
        cols = pl.ds(0, A_COLS if kind == "a" else B_COLS)
        for src, srow, rows, rel, row in parts:
            at = row
            if rel is not None:
                at = pl.multiple_of(lax.rem(y + rel, NY) * ROWS + row, 16)
            c = pltpu.make_async_copy(
                srcs[src].at[
                    pl.ds(srow, rows), pl.ds(srcs[src].shape[1] - cols.size, cols.size)
                ],
                held.at[b, pl.ds(at, rows), cols],
                in_sem.at[taken],
            )
            c.start()
            mine.append(c)
            taken += 1
        loads.append(mine)
    stores = []
    for b, (kind, zrel, _) in enumerate(blocks):
        for c in loads[b]:
            c.wait()
        zabs = lax.rem(z + zrel, NZ)
        cols = pl.ds(pl.multiple_of(zabs * BLOCK, 128), BLOCK)
        if kind == "b":
            c = pltpu.make_async_copy(
                held.at[b, :, pl.ds(0, WIDE)], down.at[cols], out_sem.at[b, 0]
            )
            c.start()
            stores.append(c)
            groups = [(WIDE, WIDE - CUT, up, CUT, 1)]
        else:
            groups = [(0, WIDE, gate, 0, 0)]
            groups += [(WIDE, CUT, up, 0, 1)] if CUT else []
        for start, width, out, row, k in groups:
            base = start if kind == "a" else start - WIDE

            def turn(i, _, start=start, base=base, b=b, step=4 * STEP):
                src = pl.multiple_of(start + i * step, STEP)
                dst = pl.multiple_of(base + i * step, STEP)
                turned[b, pl.ds(dst, step), :] = held[b, :, pl.ds(src, step)].T
                return 0

            whole, rest = divmod(width, 4 * STEP)
            lax.fori_loop(0, whole, turn, 0)
            if rest:
                last = width - rest
                turn(0, 0, start + last, base + last, b, rest)
            c = pltpu.make_async_copy(
                turned.at[b, pl.ds(base, width)],
                out.at[pl.ds(row, width), cols],
                out_sem.at[b, k],
            )
            c.start()
            stores.append(c)
    for c in stores:
        c.wait()


OUT_SHAPES = (
    jax.ShapeDtypeStruct((WIDE, NZ * BLOCK), jnp.bfloat16),
    jax.ShapeDtypeStruct((WIDE, NZ * BLOCK), jnp.bfloat16),
    jax.ShapeDtypeStruct((NZ * BLOCK, WIDE), jnp.bfloat16),
)


def placed(outs, blocks, srcs):
    first = outs is None
    n = len(blocks)
    kinds = {b[0] for b in blocks}
    cols = B_COLS if "b" in kinds else A_COLS
    tall = A_COLS if "a" in kinds else WIDE - CUT
    extra = () if first else tuple(outs)
    nbytes = n * BLOCK * cols * 4
    grant = 2 * n * BLOCK * (cols + tall) + GRANT
    return pl.pallas_call(
        functools.partial(place_body, first, blocks, len(srcs)),
        out_shape=OUT_SHAPES,
        in_specs=[ANY] * len(srcs) + [HBM] * len(extra),
        out_specs=[HBM] * 3,
        input_output_aliases={}
        if first
        else {len(srcs) + k: k for k in range(3)},
        scratch_shapes=[
            pltpu.VMEM((n, BLOCK, cols), jnp.bfloat16),
            pltpu.VMEM((n, tall, BLOCK), jnp.bfloat16),
            pltpu.SemaphoreType.DMA((sum(len(b[2]) for b in blocks),)),
            pltpu.SemaphoreType.DMA((n, 2)),
        ],
        compiler_params=pltpu.CompilerParams(vmem_limit_bytes=grant),
        cost_estimate=pl.CostEstimate(
            flops=nbytes * 200, bytes_accessed=nbytes, transcendentals=0
        ),
    )(*srcs, *extra)


def per_device(
    train_gate,
    low_gate,
    high_gate,
    train_up,
    low_up,
    high_up,
    train_down,
    low_down,
    high_down,
    norm_train,
    norm_step,
):
    z, y = "zero_0", "zero_1"
    part = 112

    gain = (norm_train + norm_step).astype(jnp.bfloat16)
    place = lax.axis_index(ZERO_TP) * gain.shape[0]
    full = lax.dynamic_update_slice(
        jnp.zeros((gain.shape[0] * 256,), jnp.bfloat16), gain, (place,)
    )
    full = lax.optimization_barrier(full)

    def sent(k, full):
        axis, step = (
            (z, -1),
            (y, -1),
            (y, 2),
            ("tp_1", 1),
            ("tp_0", 1),
            (z, -2),
            ("tp_0", 2),
            (z, 4),
        )[k]
        return shifted(full, axis, step)

    def added(full, other):
        return full + other

    def b_blocks(rels, at):
        return tuple(
            (
                "b",
                rel,
                tuple(
                    (at + s, i * ROWS, ROWS, yrel, 0)
                    for s, yrel in enumerate((0, 3, 1, 2))
                ),
            )
            for i, rel in enumerate(rels)
        )

    def a_block(rel, s):
        return ("a", rel, ((s, 0, BLOCK, None, 0),))

    own, own_b = merge_call(
        train_gate,
        low_gate.T,
        high_gate,
        train_down.T,
        high_down,
        low_down.T,
        train_up,
        low_up.T,
        high_up,
    )
    l0 = shifted(own, y, 1)
    r0 = shifted(own, y, -1)
    f1 = shifted(own_b, z, 1)
    g1 = shifted(own_b, z, -1)
    o0 = shifted(l0, y, 1)
    f2 = shifted(f1, z, 1)
    g2 = shifted(g1, z, -1)
    s1 = stacked((f1, g1), ((None, 0), (None, 96)))
    r1 = shifted(s1, y, -1)
    l1 = shifted(s1, y, 1)
    n0 = sent(0, full)
    f3 = shifted(f2, z, 1)
    g3 = shifted(g2, z, -1)
    block = stacked((own, l0, r0, o0), ((0, 0), (3, 0), (1, 0), (2, 0)), A_COLS)
    p1 = shifted(block, z, 1)
    q1 = shifted(block, z, -1)
    s2 = stacked((f2, g2), ((None, 0), (None, 96)))
    full = added(full, n0)
    n1 = sent(1, full)
    r2 = shifted(s2, y, -1)
    l2 = shifted(s2, y, 1)
    outs = placed(None, (a_block(0, 0),), (block,))
    outs = placed(outs, b_blocks((0,), 0), (own, l0, r0, o0))
    f4 = shifted(f3, z, 1)
    full = added(full, n1)
    n2 = sent(2, full)
    o1 = shifted(l1, y, 1)
    o2 = shifted(r2, y, -1)
    q2 = shifted(q1, z, -1)
    p2 = shifted(p1, z, 1)
    full = added(full, n2)
    n3 = sent(3, full)
    s3 = stacked((f3, g3, f4), ((None, 0), (None, 96), (None, 192)))
    l3 = shifted(s3, y, 1)
    r3 = shifted(s3, y, -1)
    full = added(full, n3)
    n4 = sent(4, full)
    outs = placed(outs, (a_block(7, 0), a_block(1, 1)), (p1, q1))
    full = added(full, n4)
    n5 = sent(5, full)
    q3 = shifted(q2, z, -1)
    p3 = shifted(p2, z, 1)
    outs = placed(outs, b_blocks((7, 1), 0), (s1, l1, r1, o1))
    full = added(full, n5)
    n6 = sent(6, full)
    outs = placed(outs, b_blocks((6, 2), 0), (s2, l2, r2, o2))
    full = added(full, n6)
    n7 = sent(7, full)
    b3 = shifted(r3[part:], y, -1)
    t3 = shifted(l3[:part], y, 1)
    q4 = shifted(q3[UP:], z, -1)
    p4 = shifted(p3[:UP], z, 1)
    outs = placed(outs, (a_block(6, 0), a_block(2, 1)), (p2, q2))
    outs = placed(outs, (a_block(5, 0), a_block(3, 1)), (p3, q3))
    near = [[(s, i * ROWS, ROWS, r, 0) for s, r in enumerate((0, 3, 1))] for i in range(3)]
    cut = part - ROWS
    far = (
        ((3, 0, ROWS, 2, 0),),
        ((3, ROWS, cut, 2, 0), (4, 0, ROWS - cut, 2, cut)),
        ((4, ROWS - cut, ROWS, 2, 0),),
    )
    full = added(full, n7)
    outs = placed(
        outs,
        tuple(
            ("b", rel, (*n, *f)) for rel, n, f in zip((5, 3, 4), near, far, strict=True)
        ),
        (s3, l3, r3, t3, b3),
    )
    outs = placed(
        outs, (("a", 4, ((0, 0, UP, None, 0), (1, 0, BLOCK - UP, None, UP))),), (p4, q4)
    )
    return (*outs, full)


def solution(mesh):
    finer = Mesh(mesh.devices.reshape(8, 4, 4, 2), ("zero_0", "zero_1", "tp_0", "tp_1"))
    in_specs = (
        P(ZERO, TP),
        P(ZERO, None),
        P(None, TP),
        P(ZERO, TP),
        P(ZERO, None),
        P(None, TP),
        P(TP, ZERO),
        P(TP, None),
        P(None, ZERO),
        P(ZERO_TP),
        P(ZERO_TP),
    )
    out_specs = (P(TP, None), P(TP, None), P(None, TP), P())

    step = jax.shard_map(
        per_device, mesh=finer, in_specs=in_specs, out_specs=out_specs, check_vma=False
    )
    low, wide = D_MODEL, D_INNER
    shapes = ((low, wide), (low, RANK), (RANK, wide)) * 2
    shapes += ((wide, low), (wide, RANK), (RANK, low))
    jax.eval_shape(
        step,
        *(jax.ShapeDtypeStruct(s, jnp.bfloat16) for s in shapes),
        *(jax.ShapeDtypeStruct((low,), jnp.float32) for _ in range(2)),
    )
    return step
```
